128 devices in a mesh: dp: 4 (over x_hi, core), fsdp: 8 (over z, x_lo), tensor: 4 (over y).
Axes of the slice: x: 4 (x_hi: 2, x_lo: 2; x = x_hi * 2 + x_lo), y: 4, z: 4, core: 2. Of those that a mesh axis runs over, the one named last changes fastest.
Arguments:
- tokens: bfloat16 [32, 768, 8192], P(('dp', 'fsdp'), 'tensor'), may hold values from -6 to 6
- norm_gain: float32 [8192], replicated, may hold values from 0.85 to 4
- w_qkv: bfloat16 [8192, 5120], P(('dp', 'fsdp'), 'tensor'), may hold values from -0.3 to 0.3
- a_query: bfloat16 [8192, 16], replicated, may hold values from -0.0625 to 0.0625
- query_up_adapter: bfloat16 [16, 4096], P(None, 'tensor'), may hold values from -1.5 to 1.5
- a_value: bfloat16 [8192, 16], replicated, may hold values from -0.0625 to 0.0625
- value_up_adapter: bfloat16 [16, 512], P(None, 'tensor'), may hold values from -1.5 to 1.5
- out_grad: bfloat16 [32, 768, 4096], P(('dp', 'fsdp'), 'tensor'), may hold values from -6 to 6
Outputs:
- attn_out: bfloat16 [32, 768, 4096], P(('dp', 'fsdp'), 'tensor')
- grad_a_query: float32 [8192, 16], replicated
- grad_b_query: float32 [16, 4096], P(None, 'tensor')
- grad_a_value: float32 [8192, 16], replicated
- grad_b_value: float32 [16, 512], P(None, 'tensor')
The draws below stay inside these ranges and needn't reach their ends.
All inputs are finite; a program needn't handle non-finite values.
Results may differ from the reference program's by a relative error of at most 0.015.
The reference program's roundings to bfloat16 on the way count: a program that leaves them out, or rounds other values in their place, can miss the bound.
Values may be sent and summed in bfloat16 or wider, within the bound.
No kernel may reach another device: no remote copies, remote signals or barrier semaphores. Data moves between devices by JAX's collectives and lax.ppermute only.
A program may use at most 256 MiB of HBM per device.

```python
import math
import jax
import jax.numpy as jnp
from jax import lax

D = 8192
KV = 4
HD = 128
RANK = 16
QUERY_PER_KV = 8
SEQ = 768
BATCH = 32
QCOLS = 4096
QKV = 5120


WEIGHT_EDGE = 0.296875


def draw_norm_gain(key, part):
    return 1.0 + 0.15 * jax.random.uniform(key, (D,), jnp.float32, -1.0, 1.0)


def draw_tokens(key, part):
    base = jax.random.normal(jax.random.fold_in(key, 11), (BATCH, SEQ, D), jnp.float32)
    return jnp.clip(base, -6.0, 6.0).astype(jnp.bfloat16)


def draw_w_qkv(key, part):
    base = jax.random.normal(jax.random.fold_in(key, 21), (D, QKV), jnp.float32) * (1.0 / math.sqrt(D))
    return jnp.clip(base, -WEIGHT_EDGE, WEIGHT_EDGE).astype(jnp.bfloat16)


def steps_of(stream_key, shape, pieces, least, largest):
    gain = 1.0
    for position, parts in pieces:
        heights = jax.random.uniform(jax.random.fold_in(jax.random.fold_in(stream_key, 6), position), (parts,), jnp.float32, least / len(pieces), largest / len(pieces))
        gain = gain * jnp.repeat(jnp.exp(heights), shape[position] // parts).reshape((-1,) + (1,) * (len(shape) - 1 - position))
    return gain


def normal_values(stream_key, extent, width, bound, shards=(), kind=jnp.bfloat16):
    loudness = steps_of(stream_key, extent, shards, -0.22, 0.18) if shards else 1.0
    drawn = jax.random.normal(stream_key, extent, jnp.float32) * width * loudness
    return jnp.minimum(jnp.maximum(drawn, -bound), bound).astype(kind)


def setup_inputs(seed: int = 0) -> dict:
    keys = jax.random.split(jax.random.key(seed), 9)
    tokens = draw_tokens(jax.random.fold_in(keys[8], 71), 0)
    norm_gain = draw_norm_gain(jax.random.fold_in(keys[8], 71), 0)
    w_qkv = draw_w_qkv(jax.random.fold_in(keys[8], 71), 0)
    a_query = normal_values(keys[3], (D, RANK), D ** -0.5, 0.0625)
    query_up_adapter = normal_values(keys[4], (RANK, QCOLS), RANK ** -0.5, 1.5, ((1, 4),))
    a_value = normal_values(keys[5], (D, RANK), D ** -0.5, 0.0625)
    value_up_adapter = normal_values(keys[6], (RANK, KV * HD), RANK ** -0.5, 1.5, ((1, 4),))
    out_grad = normal_values(keys[7], (BATCH, SEQ, QCOLS), 1.0, 6.0, ((0, 32), (1, 4)))
    return {"tokens": tokens, "norm_gain": norm_gain, "w_qkv": w_qkv, "a_query": a_query, "query_up_adapter": query_up_adapter, "a_value": a_value, "value_up_adapter": value_up_adapter, "out_grad": out_grad}


EPSILON = 1e-05
ADAPTER_SCALE = 2.0
ROPE_BASE = 500000.0

def normalize(own_rows, norm_gain):
    widened = own_rows.astype(jnp.float32)
    mean_square = lax.optimization_barrier(jnp.mean(widened * widened, axis=-1, keepdims=True))
    return (widened * lax.rsqrt(mean_square + EPSILON) * norm_gain).astype(jnp.bfloat16)

def rotary(heads_block):
    sequence_length = heads_block.shape[0]
    half_dim = heads_block.shape[-1] // 2
    positions = jnp.arange(sequence_length, dtype=jnp.float32)[:, None]
    inv_freq = ROPE_BASE ** (-jnp.arange(half_dim, dtype=jnp.float32) / half_dim)
    angles = positions * inv_freq
    cosine = jnp.cos(angles)[:, None, :]
    sine_table = jnp.sin(angles)[:, None, :]
    front_half = heads_block[..., :half_dim].astype(jnp.float32)
    back_half = heads_block[..., half_dim:].astype(jnp.float32)
    turned = jnp.concatenate([front_half * cosine - back_half * sine_table, back_half * cosine + front_half * sine_table], -1)
    return turned.astype(jnp.bfloat16)

def attend(query_rows, key_heads, value_rows):
    sequence_length = query_rows.shape[0]
    kv_heads = key_heads.shape[1] // HD
    rot_queries = rotary(query_rows.reshape(sequence_length, kv_heads * QUERY_PER_KV, HD))
    rot_keys = rotary(key_heads.reshape(sequence_length, kv_heads, HD))
    split_values = value_rows.reshape(sequence_length, kv_heads, HD)
    causal = jnp.arange(sequence_length)[:, None] >= jnp.arange(sequence_length)[None, :]

    def one_head(head_index):
        q_head = lax.dynamic_index_in_dim(rot_queries, head_index, 1, keepdims=False)
        k_head = lax.dynamic_index_in_dim(rot_keys, head_index // QUERY_PER_KV, 1, keepdims=False)
        v_head = lax.dynamic_index_in_dim(split_values, head_index // QUERY_PER_KV, 1, keepdims=False)
        scores = jnp.dot(q_head, k_head.T, preferred_element_type=jnp.float32) * (1.0 / math.sqrt(HD))
        scores = jnp.where(causal, scores, -1e+30)
        row_max = lax.optimization_barrier(jnp.max(scores, axis=-1, keepdims=True))
        weights = jnp.exp(scores - row_max)
        probabilities = (weights / lax.optimization_barrier(jnp.sum(weights, axis=-1, keepdims=True))).astype(jnp.bfloat16)
        return jnp.dot(probabilities, v_head, preferred_element_type=jnp.float32).astype(jnp.bfloat16)
    per_head = lax.map(one_head, jnp.arange(kv_heads * QUERY_PER_KV, dtype=jnp.int32))
    return jnp.transpose(per_head, (1, 0, 2)).reshape(sequence_length, kv_heads * QUERY_PER_KV * HD)

def reference(tokens, norm_gain, w_qkv, a_query, query_up_adapter, a_value, value_up_adapter, out_grad):
    adapters = jnp.concatenate([a_query, a_value], 1)
    narrow_rank_rows = a_query.shape[1]

    def one_sequence(pair):
        own_rows, grad_rows = pair
        normed_input = normalize(own_rows, norm_gain)
        sequence_length = normed_input.shape[0]
        projected = jnp.dot(normed_input, w_qkv, preferred_element_type=jnp.float32)
        down_projected = jnp.dot(normed_input, adapters, preferred_element_type=jnp.float32).astype(jnp.bfloat16)
        grouped_queries = projected.reshape(sequence_length, KV, QUERY_PER_KV + 2, HD)
        query_rows = (grouped_queries[:, :, :QUERY_PER_KV].reshape(sequence_length, -1) + ADAPTER_SCALE * jnp.dot(down_projected[:, :narrow_rank_rows], query_up_adapter, preferred_element_type=jnp.float32)).astype(jnp.bfloat16)
        key_heads = grouped_queries[:, :, QUERY_PER_KV].reshape(sequence_length, -1).astype(jnp.bfloat16)
        value_rows = (grouped_queries[:, :, QUERY_PER_KV + 1].reshape(sequence_length, -1) + ADAPTER_SCALE * jnp.dot(down_projected[:, narrow_rank_rows:], value_up_adapter, preferred_element_type=jnp.float32)).astype(jnp.bfloat16)
        attended, pullback = jax.vjp(attend, query_rows, key_heads, value_rows)
        query_gradient, grad_keys, value_gradient = pullback(grad_rows)
        query_up_gradient = ADAPTER_SCALE * jnp.einsum('fb,fd->bd', down_projected[:, :narrow_rank_rows], query_gradient, preferred_element_type=jnp.float32)
        value_up_gradient = ADAPTER_SCALE * jnp.einsum('fb,fd->bd', down_projected[:, narrow_rank_rows:], value_gradient, preferred_element_type=jnp.float32)
        middle_gradient = jnp.concatenate([jnp.dot(query_gradient, query_up_adapter.T, preferred_element_type=jnp.float32), jnp.dot(value_gradient, value_up_adapter.T, preferred_element_type=jnp.float32)], 1).astype(jnp.bfloat16)
        down_gradient = ADAPTER_SCALE * jnp.einsum('uh,ux->hx', normed_input, middle_gradient, preferred_element_type=jnp.float32)
        return (attended, down_gradient, query_up_gradient, value_up_gradient)
    attn_out, down_gradient, query_up_gradient, value_up_gradient = lax.map(one_sequence, (tokens, out_grad))
    down_gradient = lax.optimization_barrier(jnp.sum(down_gradient, axis=0))
    return (attn_out, down_gradient[:, :narrow_rank_rows], lax.optimization_barrier(jnp.sum(query_up_gradient, axis=0)), down_gradient[:, narrow_rank_rows:], lax.optimization_barrier(jnp.sum(value_up_gradient, axis=0)))
```

```python
import functools
import math

import jax
import jax.numpy as jnp
from jax import lax
from jax.experimental import pallas as pl
from jax.experimental.pallas import tpu as pltpu
from jax.sharding import PartitionSpec as P

HD = 128
QUERY_PER_KV = 8


EPSILON = 1e-05
ADAPTER_SCALE = 2.0
ROPE_BASE = 500000.0
WHERE = ("dp", "fsdp")
NT = (((1,), (1,)), ((), ()))
TN = (((0,), (0,)), ((), ()))


def ring(size, step):
    return [(i, (i + step) % size) for i in range(size)]


def normalize(own_rows, norm_gain):
    widened = own_rows.astype(jnp.float32)
    mean_square = jnp.mean(widened * widened, axis=-1, keepdims=True)
    return (widened * lax.rsqrt(mean_square + EPSILON) * norm_gain).astype(jnp.bfloat16)


def rotary_tables(sequence_length):
    half_dim = HD // 2
    positions = jnp.arange(sequence_length, dtype=jnp.float32)[:, None]
    inv_freq = ROPE_BASE ** (-jnp.arange(half_dim, dtype=jnp.float32) / half_dim)
    angles = positions * inv_freq
    cosine = jnp.cos(angles)
    sine = jnp.sin(angles)
    return jnp.concatenate([cosine, cosine], 1), jnp.concatenate([-sine, sine], 1)


def attention_kernel(
    block, q_ref, k_ref, v_ref, down_ref, up_q_ref, up_v_ref, grad_ref, cos_ref, sin_ref,
    out_ref, grad_b_q_ref, grad_b_v_ref, mid_ref,
    keys, keys_t, values, values_t, grad_values_t, mid_q,
):
    head = pl.program_id(0)
    last = pl.num_programs(0) - 1
    length = q_ref.shape[0]
    rank = up_q_ref.shape[0]
    f32, bf16 = jnp.float32, jnp.bfloat16
    dot = functools.partial(jnp.dot, preferred_element_type=f32)
    dot_general = functools.partial(lax.dot_general, preferred_element_type=f32)
    scale = 1.0 / math.sqrt(HD)
    to_exp2 = scale * math.log2(math.e)

    def turned(x, cosine, sine):
        return x * cosine + pltpu.roll(x, HD // 2, 1) * sine

    @pl.when(head == 0)
    def _():
        k = turned(k_ref[...].astype(bf16).astype(f32), cos_ref[...], sin_ref[...])
        keys[...] = k.astype(bf16)
        keys_t[...] = k.T.astype(bf16)
        v = v_ref[...] + ADAPTER_SCALE * dot(down_ref[:, rank:], up_v_ref[...])
        values[...] = v.astype(bf16)
        values_t[...] = v.T.astype(bf16)
        grad_values_t[...] = jnp.zeros_like(grad_values_t)
        mid_q[...] = jnp.zeros_like(mid_q)

    up_q = up_q_ref[...]
    grad_b = jnp.zeros(grad_b_q_ref.shape, f32)
    for index in range(length // block):
        rows = pl.ds(index * block, block)
        seen = (index + 1) * block
        down = down_ref[rows, :rank]
        cosine, sine = cos_ref[rows, :], sin_ref[rows, :]
        q = (q_ref[rows, :] + ADAPTER_SCALE * dot(down, up_q)).astype(bf16)
        q = turned(q.astype(f32), cosine, sine).astype(bf16)
        scores = dot(q, keys_t[:, :seen])
        row_ids = lax.broadcasted_iota(jnp.int32, (block, block), 0)
        col_ids = lax.broadcasted_iota(jnp.int32, (block, block), 1)
        diagonal = jnp.where(row_ids >= col_ids, scores[:, seen - block :], -1e30)
        if index:
            scores = jnp.concatenate([scores[:, : seen - block], diagonal], 1)
        else:
            scores = diagonal
        scores = scores * to_exp2
        weights = jnp.exp2(scores - jnp.max(scores, axis=-1, keepdims=True))
        probabilities = weights * (1.0 / jnp.sum(weights, axis=-1, keepdims=True))
        rounded = probabilities.astype(bf16)
        attended = dot(rounded, values[:seen, :])
        out_ref[rows, :] = attended.astype(bf16)
        grad_out = grad_ref[rows, :]
        grad_f32 = grad_out.astype(f32)
        grad_p = dot(grad_out, values_t[:, :seen])
        along = jnp.sum(grad_f32 * attended, axis=-1, keepdims=True)
        grad_scores = (probabilities * (grad_p - along)).astype(bf16)
        grad_q = (dot(grad_scores, keys[:seen, :]) * scale).astype(bf16).astype(f32)
        grad_q = turned(grad_q, cosine, -sine).astype(bf16)
        grad_values_t[:, :seen] += dot(grad_f32.T.astype(bf16), rounded)
        grad_b += dot_general(down, grad_q, TN)
        mid_q[rows, :] += dot_general(grad_q, up_q, NT)
    grad_b_q_ref[...] = ADAPTER_SCALE * grad_b

    @pl.when(head == last)
    def _():
        grad_v = grad_values_t[...].T.astype(bf16)
        grad_b_v_ref[...] = ADAPTER_SCALE * dot_general(down_ref[:, rank:], grad_v, TN)
        mid_ref[:, :rank] = mid_q[...]
        mid_ref[:, rank:] = dot_general(grad_v, up_v_ref[...], NT)


def attention(projected, down, up_q, up_v, grad_rows, cosine, sine):
    length = projected.shape[0]
    rank = up_q.shape[0]
    heads = up_q.shape[1] // HD
    block = 256
    whole = lambda h: (0, 0)
    column = lambda h: (0, h)
    f32, bf16 = jnp.float32, jnp.bfloat16
    return pl.pallas_call(
        functools.partial(attention_kernel, block),
        grid=(heads,),
        in_specs=[
            pl.BlockSpec((length, HD), column),
            pl.BlockSpec((length, HD), lambda h: (0, heads)),
            pl.BlockSpec((length, HD), lambda h: (0, heads + 1)),
            pl.BlockSpec((length, 2 * rank), whole),
            pl.BlockSpec((rank, HD), column),
            pl.BlockSpec((rank, HD), whole),
            pl.BlockSpec((length, HD), column),
            pl.BlockSpec((length, HD), whole),
            pl.BlockSpec((length, HD), whole),
        ],
        out_specs=[
            pl.BlockSpec((length, HD), column),
            pl.BlockSpec((rank, HD), column),
            pl.BlockSpec((rank, HD), whole),
            pl.BlockSpec((length, 2 * rank), whole),
        ],
        out_shape=[
            jax.ShapeDtypeStruct((length, heads * HD), bf16),
            jax.ShapeDtypeStruct((rank, heads * HD), f32),
            jax.ShapeDtypeStruct((rank, HD), f32),
            jax.ShapeDtypeStruct((length, 2 * rank), f32),
        ],
        scratch_shapes=[
            pltpu.VMEM((length, HD), bf16),
            pltpu.VMEM((HD, length), bf16),
            pltpu.VMEM((length, HD), bf16),
            pltpu.VMEM((HD, length), bf16),
            pltpu.VMEM((HD, length), f32),
            pltpu.VMEM((length, rank), f32),
        ],
        compiler_params=pltpu.CompilerParams(dimension_semantics=("arbitrary",)),
        name="attention",
    )(projected, projected, projected, down, up_q, up_v, grad_rows, cosine, sine)


def local(tokens, norm_gain, w_qkv, a_query, query_up_adapter, a_value, value_up_adapter, out_grad):
    f32, bf16 = jnp.float32, jnp.bfloat16
    size = lax.axis_size("tensor")
    me = lax.axis_index("tensor")
    rank = a_query.shape[1]
    own = out_grad.shape[1]
    length = own * size
    q_cols = query_up_adapter.shape[1]

    weights = lax.all_gather(w_qkv, WHERE, axis=0, tiled=True)
    grad_rows = lax.all_to_all(out_grad[0], "tensor", split_axis=1, concat_axis=0, tiled=True)

    normed = normalize(tokens[0], norm_gain)
    ahead, behind = ring(size, 1), ring(size, -1)
    from_left = lax.ppermute(normed, "tensor", ahead)
    from_right = lax.ppermute(normed, "tensor", behind)
    half = own // 2
    far_top = lax.ppermute(from_left[:half], "tensor", ahead)
    far_low = lax.ppermute(from_right[half:], "tensor", behind)
    gathered = jnp.zeros((length, normed.shape[1]), bf16)
    for rows, place in (
        (normed, me * own),
        (from_left, (me + size - 1) % size * own),
        (from_right, (me + 1) % size * own),
        (far_top, (me + 2) % size * own),
        (far_low, (me + 2) % size * own + half),
    ):
        gathered = lax.dynamic_update_slice(gathered, rows, (place, 0))

    adapters = jnp.concatenate([a_query, a_value], 1)
    down = jnp.dot(gathered, adapters, preferred_element_type=f32).astype(bf16)
    projected = jnp.dot(gathered, weights, preferred_element_type=f32)
    cosine, sine = rotary_tables(length)
    attended, grad_b_q, grad_b_v, mid = attention(
        projected, down, query_up_adapter, value_up_adapter, grad_rows, cosine, sine
    )
    out_rows = lax.all_to_all(attended, "tensor", split_axis=0, concat_axis=1, tiled=True)

    spread = jnp.broadcast_to(mid[None], (size, *mid.shape))
    mid_sum = lax.all_to_all(spread, "tensor", 0, 0, tiled=True).sum(axis=0).astype(bf16)
    part = normed.shape[1] // size
    features = lax.dynamic_slice(gathered, (0, me * part), (length, part))
    grad_a = ADAPTER_SCALE * lax.dot_general(mid_sum, features, TN, preferred_element_type=f32)

    groups = lax.axis_size(WHERE)
    packed = jnp.concatenate(
        [
            grad_a.reshape(groups, -1),
            grad_b_q.reshape(groups, -1),
            grad_b_v.reshape(groups, -1),
        ],
        1,
    )
    width = packed.shape[1]
    padded = -(-width // 1024) * 1024
    packed = jnp.pad(packed, ((0, 0), (0, padded - width))).reshape(groups, 8, padded // 8)
    summed = lax.all_to_all(packed, WHERE, 0, 0, tiled=True).sum(axis=0)
    shared = lax.all_gather(summed, WHERE, axis=0, tiled=False).reshape(groups, padded)
    n_a, n_q, n_v = grad_a.size // groups, grad_b_q.size // groups, grad_b_v.size // groups
    grad_a = shared[:, :n_a].reshape(grad_a.shape)
    grad_b_q = shared[:, n_a : n_a + n_q].reshape(grad_b_q.shape)
    grad_b_v = shared[:, n_a + n_q : n_a + n_q + n_v].reshape(grad_b_v.shape)
    grad_a = lax.all_gather(grad_a, "tensor", axis=1, tiled=True)
    return out_rows[None], grad_a[:rank].T, grad_b_q, grad_a[rank:].T, grad_b_v


def solution(mesh):
    return jax.shard_map(
        local,
        mesh=mesh,
        in_specs=(
            P(("dp", "fsdp"), "tensor", None),
            P(),
            P(("dp", "fsdp"), "tensor"),
            P(),
            P(None, "tensor"),
            P(),
            P(None, "tensor"),
            P(("dp", "fsdp"), "tensor", None),
        ),
        out_specs=(
            P(("dp", "fsdp"), "tensor", None),
            P(),
            P(None, "tensor"),
            P(),
            P(None, "tensor"),
        ),
        check_vma=False,
    )
```

```python
import functools
import math

import jax
import jax.numpy as jnp
from jax import lax
from jax.experimental import pallas as pl
from jax.experimental.pallas import tpu as pltpu
from jax.sharding import PartitionSpec as P


HD = 128


EPSILON = 1e-05
ADAPTER_SCALE = 2.0
ROPE_BASE = 500000.0
WHERE = ("dp", "fsdp")
NT = (((1,), (1,)), ((), ()))
TN = (((0,), (0,)), ((), ()))


def ring(size, step):
    return [(i, (i + step) % size) for i in range(size)]


def normalize_kernel(rows_ref, gain_ref, out_ref):
    widened = rows_ref[...].astype(jnp.float32)
    mean_square = jnp.mean(widened * widened, axis=-1, keepdims=True)
    normed = widened * lax.rsqrt(mean_square + EPSILON) * gain_ref[...]
    out_ref[...] = normed.astype(jnp.bfloat16)


def normalize(rows, norm_gain, first, count, block):
    width = rows.shape[1]
    return pl.pallas_call(
        normalize_kernel,
        grid=(count // block,),
        in_specs=[
            pl.BlockSpec((block, width), lambda i: (first // block + i, 0)),
            pl.BlockSpec((1, width), lambda i: (0, 0)),
        ],
        out_specs=pl.BlockSpec((block, width), lambda i: (i, 0)),
        out_shape=jax.ShapeDtypeStruct((count, width), jnp.bfloat16),
        compiler_params=pltpu.CompilerParams(dimension_semantics=("arbitrary",)),
        name="normalize",
    )(rows, norm_gain.reshape(1, width))


AHEAD = 3


def project_kernel(turns, n_rows, starts_ref, *refs):
    n_pieces = sum(len(turn) for turn in turns)
    rows_refs, pieces = refs[:n_rows], refs[n_rows : n_rows + n_pieces]
    out_ref, rows, weights, rows_sem, weights_sem = refs[n_rows + n_pieces :]
    deep = weights.shape[0] // len(turns)
    depth = weights.shape[0] // starts_ref.shape[0]
    blocks = deep // depth

    def fetch(turn):
        place = turn * deep
        for piece, count in turns[turn]:
            pltpu.make_async_copy(
                pieces[piece], weights.at[pl.ds(place, count)], weights_sem.at[turn]
            ).start()
            place += count

    row_copies = []
    for index, ref in enumerate(rows_refs):
        count = ref.shape[0]
        row_copies.append(
            pltpu.make_async_copy(
                ref, rows.at[pl.ds(index * count, count)], rows_sem.at[index]
            )
        )
        row_copies[-1].start()
    for turn in range(AHEAD):
        fetch(turn)
    out_ref[...] = jnp.zeros_like(out_ref)
    for copy in row_copies:
        copy.wait()

    def step(turn, carry):
        for later in range(AHEAD, len(turns)):

            @pl.when(turn + AHEAD == later)
            def _(later=later):
                fetch(later)

        here = weights.at[pl.ds(pl.multiple_of(turn * deep, deep), deep)]
        pltpu.make_async_copy(here, here, weights_sem.at[turn]).wait()
        columns = [
            rows[:, pl.ds(pl.multiple_of(starts_ref[turn * blocks + k], depth), depth)]
            for k in range(blocks)
        ]
        out_ref[...] += jnp.dot(
            jnp.concatenate(columns, 1), here[...], preferred_element_type=jnp.float32
        )
        return carry

    lax.fori_loop(0, len(turns), step, 0)


def project(rows, starts, pieces, blocks):
    depth, cols = pieces[0].shape[1:]
    sizes = [piece.shape[0] for piece in pieces]
    count, width = sum(part.shape[0] for part in rows), rows[0].shape[1]
    anywhere = pl.BlockSpec(memory_space=pl.ANY)
    turns, filled = [[]], 0
    for index, size in enumerate(sizes):
        if filled == blocks:
            turns.append([])
            filled = 0
        turns[-1].append((index, size * depth))
        filled += size
    return pl.pallas_call(
        functools.partial(project_kernel, turns, len(rows)),
        grid_spec=pltpu.PrefetchScalarGridSpec(
            num_scalar_prefetch=1,
            grid=(1,),
            in_specs=[anywhere] * (len(rows) + len(pieces)),
            out_specs=pl.BlockSpec((count, cols), lambda i, p: (0, 0)),
            scratch_shapes=[
                pltpu.VMEM((count, width), jnp.bfloat16),
                pltpu.VMEM((sum(sizes) * depth, cols), jnp.bfloat16),
                pltpu.SemaphoreType.DMA((len(rows),)),
                pltpu.SemaphoreType.DMA((len(turns),)),
            ],
        ),
        out_shape=jax.ShapeDtypeStruct((count, cols), jnp.float32),
        name="project",
    )(starts, *rows, *[piece.reshape(-1, cols) for piece in pieces])


def rotary_tables(sequence_length):
    half_dim = HD // 2
    positions = jnp.arange(sequence_length, dtype=jnp.float32)[:, None]
    inv_freq = ROPE_BASE ** (-jnp.arange(half_dim, dtype=jnp.float32) / half_dim)
    angles = positions * inv_freq
    cosine = jnp.cos(angles)
    sine = jnp.sin(angles)
    return jnp.concatenate([cosine, cosine], 1), jnp.concatenate([-sine, sine], 1)


def attention_kernel(
    block, places_ref,
    q_near_ref, q_far_ref, k_near_ref, k_far_ref, v_near_ref, v_far_ref,
    down_own, down_left, down_right, down_far, up_q_ref, up_v_ref, cos_ref, sin_ref,
    grad_own, grad_left, grad_right, grad_top, grad_low,
    out_own, out_left, out_right, out_top, out_low, grad_b_q_ref, grad_b_v_ref, mid_ref,
    queries, grads, outs, keys, keys_t, values, values_t, downs, grad_values_t, mid_q,
):
    head = pl.program_id(0)
    last = pl.num_programs(0) - 1
    length = outs.shape[0]
    own = q_far_ref.shape[0]
    rank = up_q_ref.shape[0]
    f32, bf16 = jnp.float32, jnp.bfloat16
    dot = functools.partial(jnp.dot, preferred_element_type=f32)
    dot_general = functools.partial(lax.dot_general, preferred_element_type=f32)
    scale = 1.0 / math.sqrt(HD)
    to_exp2 = scale * math.log2(math.e)

    def turned(x, cosine, sine):
        return x * cosine + pltpu.roll(x, HD // 2, 1) * sine

    def each_chunk(near_ref, far_ref):
        for index in range(length // own):
            rows = pl.ds(pl.multiple_of(places_ref[index] * own, own), own)
            if (index + 1) * own <= near_ref.shape[0]:
                yield rows, near_ref[index * own : (index + 1) * own, :]
            else:
                yield rows, far_ref[...]

    @pl.when(head == 0)
    def _():
        for index, down in enumerate((down_own, down_left, down_right, down_far)):
            rows = pl.ds(pl.multiple_of(places_ref[index] * own, own), own)
            downs[rows, :] = down[...]
        for rows, k in each_chunk(k_near_ref, k_far_ref):
            k = turned(k.astype(bf16).astype(f32), cos_ref[rows, :], sin_ref[rows, :])
            keys[rows, :] = k.astype(bf16)
        for rows, v in each_chunk(v_near_ref, v_far_ref):
            v = v + ADAPTER_SCALE * dot(downs[rows, rank:], up_v_ref[...])
            values[rows, :] = v.astype(bf16)
        keys_t[...] = keys[...].astype(f32).T.astype(bf16)
        values_t[...] = values[...].astype(f32).T.astype(bf16)
        grad_values_t[...] = jnp.zeros_like(grad_values_t)
        mid_q[...] = jnp.zeros_like(mid_q)

    up_q = up_q_ref[...]
    for rows, q in each_chunk(q_near_ref, q_far_ref):
        q = (q + ADAPTER_SCALE * dot(downs[rows, :rank], up_q)).astype(bf16)
        queries[rows, :] = turned(q.astype(f32), cos_ref[rows, :], sin_ref[rows, :]).astype(bf16)
    half = own // 2

    def spots():
        starts = [pl.multiple_of(places_ref[index] * own, own) for index in range(4)]
        low = pl.multiple_of(starts[3] + half, half)
        return [pl.ds(start, own) for start in starts[:3]] + [pl.ds(starts[3], half), pl.ds(low, half)]

    for rows, part in zip(spots(), (grad_own, grad_left, grad_right, grad_top, grad_low)):
        grads[rows, :] = part[...]
    spans = [(pl.ds(i * block, block), (i + 1) * block) for i in reversed(range(length // block))]
    row_ids = lax.broadcasted_iota(jnp.int32, (block, block), 0)
    col_ids = lax.broadcasted_iota(jnp.int32, (block, block), 1)
    causal = row_ids >= col_ids
    all_scores = [dot(queries[rows, :], keys_t[:, :seen]) for rows, seen in spans]
    softmaxes = []
    for (rows, seen), scores in zip(spans, all_scores):
        diagonal = jnp.where(causal, scores[:, seen - block :], -1e30)
        if seen > block:
            scores = jnp.concatenate([scores[:, : seen - block], diagonal], 1)
        else:
            scores = diagonal
        weights = jnp.exp2((scores - jnp.max(scores, axis=-1, keepdims=True)) * to_exp2)
        inverse = 1.0 / jnp.sum(weights, axis=-1, keepdims=True)
        softmaxes.append((weights, inverse, weights.astype(bf16)))
    grad_qs = []
    for (rows, seen), (weights, inverse, rounded), grad_p in zip(spans, softmaxes, [None] * 3):
        attended = dot(rounded, values[:seen, :]) * inverse
        outs[rows, :] = attended.astype(bf16)
        grad_f32 = grads[rows, :].astype(f32)
        along = jnp.sum(grad_f32 * attended, axis=-1, keepdims=True)
        grad_p = dot(grads[rows, :], values_t[:, :seen])
        grad_scores = (weights * (grad_p - along)).astype(bf16)
        grad_qs.append(dot(grad_scores, keys[:seen, :]) * (inverse * scale))
        grad_values_t[:, :seen] += dot((grad_f32 * inverse).T.astype(bf16), rounded)
    grad_b = jnp.zeros(grad_b_q_ref.shape, f32)
    for (rows, seen), grad_q in zip(spans, grad_qs):
        grad_q = turned(grad_q.astype(bf16).astype(f32), cos_ref[rows, :], -sin_ref[rows, :])
        grad_q = grad_q.astype(bf16)
        grad_b += dot_general(downs[rows, :rank], grad_q, TN)
        mid_q[:, rows] += dot_general(up_q, grad_q, NT)
    grad_b_q_ref[...] = ADAPTER_SCALE * grad_b
    for rows, part in zip(spots(), (out_own, out_left, out_right, out_top, out_low)):
        part[...] = outs[rows, :]

    @pl.when(head == last)
    def _():
        grad_v = grad_values_t[...].T.astype(bf16)
        grad_b_v_ref[...] = ADAPTER_SCALE * dot_general(downs[:, rank:], grad_v, TN)
        mid_ref[:rank, :] = mid_q[...]
        mid_ref[rank:, :] = dot_general(up_v_ref[...], grad_v, NT)


def attention(places, near, far, downs, up_q, up_v, grads, cosine, sine):
    close, own = near.shape[0], far.shape[0]
    length = close + own
    rank = up_q.shape[0]
    heads = up_q.shape[1] // HD
    whole = lambda h, p: (0, 0)
    column = lambda h, p: (0, h)
    f32, bf16 = jnp.float32, jnp.bfloat16
    pairs = []
    for index in (column, lambda h, p: (0, heads), lambda h, p: (0, heads + 1)):
        pairs += [pl.BlockSpec((close, HD), index), pl.BlockSpec((own, HD), index)]
    return pl.pallas_call(
        functools.partial(attention_kernel, 256),
        grid_spec=pltpu.PrefetchScalarGridSpec(
            num_scalar_prefetch=1,
            grid=(heads,),
            in_specs=pairs
            + [
                *[pl.BlockSpec((own, 2 * rank), whole)] * 4,
                pl.BlockSpec((rank, HD), column),
                pl.BlockSpec((rank, HD), whole),
                pl.BlockSpec((length, HD), whole),
                pl.BlockSpec((length, HD), whole),
            ]
            + [pl.BlockSpec((part.shape[0], HD), column) for part in grads],
            out_specs=[pl.BlockSpec((part.shape[0], HD), column) for part in grads]
            + [
                pl.BlockSpec((rank, HD), column),
                pl.BlockSpec((rank, HD), whole),
                pl.BlockSpec((2 * rank, length), whole),
            ],
            scratch_shapes=[
                pltpu.VMEM((length, HD), bf16),
                pltpu.VMEM((length, HD), bf16),
                pltpu.VMEM((length, HD), bf16),
                pltpu.VMEM((length, HD), bf16),
                pltpu.VMEM((HD, length), bf16),
                pltpu.VMEM((length, HD), bf16),
                pltpu.VMEM((HD, length), bf16),
                pltpu.VMEM((length, 2 * rank), bf16),
                pltpu.VMEM((HD, length), f32),
                pltpu.VMEM((rank, length), f32),
            ],
        ),
        out_shape=[jax.ShapeDtypeStruct(part.shape, bf16) for part in grads]
        + [
            jax.ShapeDtypeStruct((rank, heads * HD), f32),
            jax.ShapeDtypeStruct((rank, HD), f32),
            jax.ShapeDtypeStruct((2 * rank, length), f32),
        ],
        compiler_params=pltpu.CompilerParams(dimension_semantics=("arbitrary",)),
        name="attention",
    )(
        places, near, far, near, far, near, far,
        *downs, up_q, up_v, cosine, sine, *grads,
    )


def coordinates():
    dp, fsdp = lax.axis_index("dp"), lax.axis_index("fsdp")
    return dp // 2 * 2 + fsdp % 2, fsdp // 2, dp % 2


def position(x, z, c):
    return (x // 2 * 2 + c) * 8 + z * 2 + x % 2


def moves(dx=0, dz=0, dc=0):
    return [
        (position(x, z, c), position((x + dx) % 4, (z + dz) % 4, (c + dc) % 2))
        for x in range(4)
        for z in range(4)
        for c in range(2)
    ]


def send(array, dx=0, dz=0, dc=0):
    return lax.ppermute(array, WHERE, moves(dx, dz, dc))


def around(array, **step):
    back = {axis: -size for axis, size in step.items()}
    before, after = send(array, **step), send(array, **back)
    half = array.shape[0] // 2
    top, low = send(before[:half], **step), send(after[half:], **back)
    return before, after, top, low


def gather_weights(shard, x, z, c):
    rows, _ = shard.shape
    half = rows // 2

    def joined(own, pieces, at):
        line = jnp.zeros((4, *own.shape), own.dtype)
        before, after, top, low = pieces
        cut = own.shape[0] // 2
        for piece, index, row in (
            (own, at, 0), (before, at - 1, 0), (after, at + 1, 0), (top, at + 2, 0), (low, at + 2, cut),
        ):
            line = lax.dynamic_update_slice(line, piece[None], (index % 4, row, 0))
        return line

    along_x = joined(shard[:half], around(shard[:half], dx=1), x)
    along_z = joined(shard[half:], around(shard[half:], dz=1), z)
    from_z = around(along_x, dz=1)
    from_x = around(along_z, dx=1)
    pieces, starts = [], []

    def add(piece, blocks, core, second):
        pieces.append(piece)
        starts.extend(position(x, z, core) * rows + second * half for x, z in blocks)

    spans = (range(4), range(4), range(4), range(2), range(2, 4))
    turns = (0, -1, 1, 2, 2)
    for k in range(5):
        for other in (False, True):
            core = 1 - c if other else c
            piece = (along_x, *from_z)[k]
            at = (z + turns[k]) % 4
            piece = send(piece, dc=1) if other else piece
            add(piece, [(i, at) for i in spans[k]], core, 0)
            piece = (along_z, *from_x)[k]
            at = (x + turns[k]) % 4
            piece = send(piece, dc=1) if other else piece
            add(piece, [(at, i) for i in spans[k]], core, 1)
    return pieces, jnp.stack([jnp.asarray(start, jnp.int32) for start in starts])


def pick(array, index):
    return lax.dynamic_index_in_dim(array, index, 0, keepdims=False)


def placed(array, at, parts):
    size = len(parts) + 1
    line = jnp.zeros((size, *array.shape), array.dtype)
    for k, part in enumerate((array, *parts)):
        line = lax.dynamic_update_index_in_dim(line, part, (at + size - k) % size, 0)
    return line


def reduce(keep, give, x, z):
    total = keep + send(give, dc=1)
    others = [send(pick(total, (x + k) % 4), dx=k) for k in (1, 2, 3)]
    total = (pick(total, x) + others[0] + others[1] + others[2]).astype(jnp.bfloat16)
    parts = placed(total, z, [send(total, dz=k) for k in (1, 2, 3)])
    return parts.astype(jnp.float32).sum(axis=0).astype(jnp.bfloat16)


def all_gather(mine, me, x, c):
    first = mine[..., :SHARED]
    first = placed(first, me, [lax.ppermute(first, "tensor", ring(4, k)) for k in (1, 2, 3)])
    mine = jnp.concatenate([*first, mine[..., SHARED:]], -1)
    mine = placed(mine, x, [send(mine, dx=k) for k in (1, 2, 3)])
    return placed(mine, c, [send(mine, dc=1)])


SHARED, LANES = 256, 384


def feature_kernel(
    places_ref, mid0, mid1, mid2, mid3, *refs
):
    parts, (grad_q_ref, grad_v_ref, keep_ref, give_ref, mids, packed) = refs[:-6], refs[-6:]
    f32, bf16 = jnp.float32, jnp.bfloat16
    half = parts[0].shape[0]
    mids[...] = (mid0[...] + mid1[...] + mid2[...] + mid3[...]).T.astype(bf16)
    total = jnp.zeros((mids.shape[1], parts[0].shape[1]), f32)
    for index, part in enumerate(parts):
        start = places_ref[index // 2] * 2 * half + index % 2 * half
        mid = mids[pl.ds(pl.multiple_of(start, half), half), :]
        total = total + lax.dot_general(mid, part[...], TN, preferred_element_type=f32)
    total = total * ADAPTER_SCALE
    packed[:, :, SHARED:] = jnp.zeros((32, 8, LANES - SHARED), f32)
    for chunk in range(32):
        top, left = chunk // 8, chunk % 8
        packed[chunk, :, :SHARED] = total[top * 8 : top * 8 + 8, left * 256 : left * 256 + 256]
        packed[chunk, :4, SHARED:] = grad_q_ref[top * 4 : top * 4 + 4, left * 128 : left * 128 + 128]
        if chunk < 16:
            packed[chunk, 4:5, SHARED:] = grad_v_ref[chunk : chunk + 1, :]
    core = places_ref[4]
    keep_ref[...] = packed[pl.ds(core * 16, 16)]
    give_ref[...] = packed[pl.ds((1 - core) * 16, 16)]


def feature_gradient(places, mids, parts, grad_b_q, grad_b_v):
    half, width = parts[0].shape
    part = width // 4
    whole = lambda i, p: (0, 0)
    out = pl.BlockSpec((16, 8, LANES), lambda i, p: (0, 0, 0))
    keep, give = pl.pallas_call(
        feature_kernel,
        grid_spec=pltpu.PrefetchScalarGridSpec(
            num_scalar_prefetch=1,
            grid=(1,),
            in_specs=[
                *[pl.BlockSpec(mids[0].shape, whole)] * 4,
                *[pl.BlockSpec((half, part), lambda i, p: (0, p[0]))] * len(parts),
                pl.BlockSpec(grad_b_q.shape, whole),
                pl.BlockSpec(grad_b_v.shape, whole),
            ],
            out_specs=[out, out],
            scratch_shapes=[
                pltpu.VMEM(mids[0].shape[::-1], jnp.bfloat16),
                pltpu.VMEM((32, 8, LANES), jnp.float32),
            ],
        ),
        out_shape=[jax.ShapeDtypeStruct((16, 8, LANES), jnp.float32)] * 2,
        name="features",
    )(places, *mids, *parts, grad_b_q, grad_b_v)
    return keep.reshape(4, 4, 8, LANES), give.reshape(4, 4, 8, LANES)


def unpack_kernel(all_ref, a_query_ref, a_value_ref, grad_q_ref, grad_v_ref):
    f32 = jnp.float32
    for chunk in range(32):
        top, left = chunk // 8, chunk % 8
        target = (a_query_ref, a_value_ref)[top // 2]
        row = top % 2 * 8
        for y in range(4):
            lane = y * 2048 + left * 256
            piece = all_ref[chunk, :, y * SHARED : y * SHARED + SHARED].astype(f32)
            target[row : row + 8, lane : lane + 256] = piece
        mine = all_ref[chunk, :, 4 * SHARED :].astype(f32)
        grad_q_ref[top * 4 : top * 4 + 4, left * 128 : left * 128 + 128] = mine[:4]
        if chunk < 16:
            grad_v_ref[chunk : chunk + 1, :] = mine[4:5]


def unpack(everything, rank):
    everything = everything.reshape(32, 8, -1)
    shapes = ((rank, 8192), (rank, 8192), (rank, 1024), (rank, 128))
    return pl.pallas_call(
        unpack_kernel,
        out_shape=[jax.ShapeDtypeStruct(s, jnp.float32) for s in shapes],
        name="unpack",
    )(everything)


def local(tokens, norm_gain, w_qkv, a_query, query_up_adapter, a_value, value_up_adapter, out_grad):
    f32, bf16 = jnp.float32, jnp.bfloat16
    size = lax.axis_size("tensor")
    me = lax.axis_index("tensor")
    rank = a_query.shape[1]
    own = out_grad.shape[1]
    half = own // 2
    x, z, c = coordinates()
    ahead, behind = ring(size, 1), ring(size, -1)
    right, left, across = (me + 1) % size, (me + size - 1) % size, (me + 2) % size

    def along(array, pairs):
        return lax.ppermute(array, "tensor", pairs)

    width = out_grad.shape[2] // size
    group = lambda at: lax.dynamic_slice(out_grad[0], (0, at * width), (own, width))
    cross = group(across)
    grads = (
        group(me),
        along(group(right), ahead),
        along(group(left), behind),
        along(along(cross[:half], ahead), ahead),
        along(along(cross[half:], behind), behind),
    )
    pieces, starts = gather_weights(w_qkv, x, z, c)

    top = normalize(tokens[0], norm_gain, 0, half, 32)
    low = normalize(tokens[0], norm_gain, half, half, 32)
    left_top = along(top, ahead)
    right_low = along(low, behind)
    left_low = along(low, ahead)
    right_top = along(top, behind)
    far_top = along(left_top, ahead)
    far_low = along(right_low, behind)
    near, far = (top, low, left_top, left_low, right_top, right_low), (far_top, far_low)

    adapters = jnp.concatenate([a_query, a_value], 1)
    down = jnp.concatenate(
        [jnp.dot(part, adapters, preferred_element_type=f32).astype(bf16) for part in (top, low)]
    )
    downs = [down] + [along(down, ring(size, step)) for step in (1, -1, 2)]
    near_projected = project(near, starts, pieces, 4)
    far_projected = project(far, starts, pieces, 8)
    places = jnp.stack([me, left, right, across, c]).astype(jnp.int32)
    cosine, sine = rotary_tables(own * size)
    mine, for_left, for_right, for_top, for_low, grad_b_q, grad_b_v, mid = attention(
        places, near_projected, far_projected, downs,
        query_up_adapter, value_up_adapter, grads, cosine, sine,
    )

    mids = [mid] + [along(mid, ring(size, k)) for k in (1, 2, 3)]
    out = jnp.zeros((own, out_grad.shape[2]), bf16)
    for piece, row, source in (
        (mine, 0, me),
        (along(for_right, ahead), 0, left),
        (along(for_left, behind), 0, right),
        (along(along(for_top, ahead), ahead), 0, across),
        (along(along(for_low, behind), behind), half, across),
    ):
        out = lax.dynamic_update_slice(out, piece, (row, source * width))
    keep, give = feature_gradient(places, mids, near + far, grad_b_q, grad_b_v)
    summed = reduce(keep, give, x, z)
    grad_a_q, grad_a_v, grad_b_q, grad_b_v = unpack(all_gather(summed, me, x, c), rank)
    return out[None], grad_a_q.T, grad_b_q, grad_a_v.T, grad_b_v


def solution(mesh):
    return jax.shard_map(
        local,
        mesh=mesh,
        in_specs=(
            P(("dp", "fsdp"), "tensor", None),
            P(),
            P(("dp", "fsdp"), "tensor"),
            P(),
            P(None, "tensor"),
            P(),
            P(None, "tensor"),
            P(("dp", "fsdp"), "tensor", None),
        ),
        out_specs=(
            P(("dp", "fsdp"), "tensor", None),
            P(),
            P(None, "tensor"),
            P(),
            P(None, "tensor"),
        ),
        check_vma=False,
    )
```

```python
import functools
import math

import jax
import jax.numpy as jnp
from jax import lax
from jax.experimental import pallas as pl
from jax.experimental.pallas import tpu as pltpu
from jax.sharding import PartitionSpec as P


HD = 128


EPSILON = 1e-05
ADAPTER_SCALE = 2.0
ROPE_BASE = 500000.0
WHERE = ("dp", "fsdp")
NT = (((1,), (1,)), ((), ()))
TN = (((0,), (0,)), ((), ()))


def ring(size, step):
    return [(i, (i + step) % size) for i in range(size)]


def normalize_kernel(rows_ref, gain_ref, out_ref):
    widened = rows_ref[...].astype(jnp.float32)
    mean_square = jnp.mean(widened * widened, axis=-1, keepdims=True)
    normed = widened * lax.rsqrt(mean_square + EPSILON) * gain_ref[...]
    out_ref[...] = normed.astype(jnp.bfloat16)


def normalize(rows, norm_gain, first, count, block):
    width = rows.shape[1]
    return pl.pallas_call(
        normalize_kernel,
        grid=(count // block,),
        in_specs=[
            pl.BlockSpec((block, width), lambda i: (first // block + i, 0)),
            pl.BlockSpec((1, width), lambda i: (0, 0)),
        ],
        out_specs=pl.BlockSpec((block, width), lambda i: (i, 0)),
        out_shape=jax.ShapeDtypeStruct((count, width), jnp.bfloat16),
        compiler_params=pltpu.CompilerParams(dimension_semantics=("arbitrary",)),
        name="normalize",
    )(rows, norm_gain.reshape(1, width))


AHEAD = 3


def project_kernel(turns, n_rows, starts_ref, *refs):
    n_pieces = sum(len(turn) for turn in turns)
    rows_refs, pieces = refs[:n_rows], refs[n_rows : n_rows + n_pieces]
    out_ref, rows, weights, rows_sem, weights_sem = refs[n_rows + n_pieces :]
    deep = weights.shape[0] // len(turns)
    depth = weights.shape[0] // starts_ref.shape[0]
    blocks = deep // depth

    def fetch(turn):
        place = turn * deep
        for piece, count in turns[turn]:
            pltpu.make_async_copy(
                pieces[piece], weights.at[pl.ds(place, count)], weights_sem.at[turn]
            ).start()
            place += count

    row_copies = []
    for index, ref in enumerate(rows_refs):
        count = ref.shape[0]
        row_copies.append(
            pltpu.make_async_copy(
                ref, rows.at[pl.ds(index * count, count)], rows_sem.at[index]
            )
        )
        row_copies[-1].start()
    for turn in range(AHEAD):
        fetch(turn)
    out_ref[...] = jnp.zeros_like(out_ref)
    for copy in row_copies:
        copy.wait()

    def step(turn, carry):
        for later in range(AHEAD, len(turns)):

            @pl.when(turn + AHEAD == later)
            def _(later=later):
                fetch(later)

        here = weights.at[pl.ds(pl.multiple_of(turn * deep, deep), deep)]
        pltpu.make_async_copy(here, here, weights_sem.at[turn]).wait()
        columns = [
            rows[:, pl.ds(pl.multiple_of(starts_ref[turn * blocks + k], depth), depth)]
            for k in range(blocks)
        ]
        out_ref[...] += jnp.dot(
            jnp.concatenate(columns, 1), here[...], preferred_element_type=jnp.float32
        )
        return carry

    lax.fori_loop(0, len(turns), step, 0)


def project(rows, starts, pieces, blocks):
    depth, cols = pieces[0].shape[1:]
    sizes = [piece.shape[0] for piece in pieces]
    count, width = sum(part.shape[0] for part in rows), rows[0].shape[1]
    anywhere = pl.BlockSpec(memory_space=pl.ANY)
    turns, filled = [[]], 0
    for index, size in enumerate(sizes):
        if filled == blocks:
            turns.append([])
            filled = 0
        turns[-1].append((index, size * depth))
        filled += size
    return pl.pallas_call(
        functools.partial(project_kernel, turns, len(rows)),
        grid_spec=pltpu.PrefetchScalarGridSpec(
            num_scalar_prefetch=1,
            grid=(1,),
            in_specs=[anywhere] * (len(rows) + len(pieces)),
            out_specs=pl.BlockSpec((count, cols), lambda i, p: (0, 0)),
            scratch_shapes=[
                pltpu.VMEM((count, width), jnp.bfloat16),
                pltpu.VMEM((sum(sizes) * depth, cols), jnp.bfloat16),
                pltpu.SemaphoreType.DMA((len(rows),)),
                pltpu.SemaphoreType.DMA((len(turns),)),
            ],
        ),
        out_shape=jax.ShapeDtypeStruct((count, cols), jnp.float32),
        name="project",
    )(starts, *rows, *[piece.reshape(-1, cols) for piece in pieces])


def rotary_tables(sequence_length):
    half_dim = HD // 2
    positions = jnp.arange(sequence_length, dtype=jnp.float32)[:, None]
    inv_freq = ROPE_BASE ** (-jnp.arange(half_dim, dtype=jnp.float32) / half_dim)
    angles = positions * inv_freq
    cosine = jnp.cos(angles)
    sine = jnp.sin(angles)
    return jnp.concatenate([cosine, cosine], 1), jnp.concatenate([-sine, sine], 1)


def attention_kernel(
    block, places_ref,
    q_near_ref, q_far_ref, k_near_ref, k_far_ref, v_near_ref, v_far_ref,
    down_own, down_left, down_right, down_far, up_q_ref, up_v_ref, cos_ref, sin_ref,
    grad_own, grad_left, grad_right, grad_top, grad_low,
    out_own, out_left, out_right, out_top, out_low, grad_b_q_ref, grad_b_v_ref, mid_ref,
    queries, grads, outs, keys, keys_t, values, values_t, downs, grad_values_t, mid_q,
):
    head = pl.program_id(0)
    last = pl.num_programs(0) - 1
    length = outs.shape[0]
    own = q_far_ref.shape[0]
    rank = up_q_ref.shape[0]
    f32, bf16 = jnp.float32, jnp.bfloat16
    dot = functools.partial(jnp.dot, preferred_element_type=f32)
    dot_general = functools.partial(lax.dot_general, preferred_element_type=f32)
    scale = 1.0 / math.sqrt(HD)
    to_exp2 = scale * math.log2(math.e)

    def turned(x, cosine, sine):
        return x * cosine + pltpu.roll(x, HD // 2, 1) * sine

    def each_chunk(near_ref, far_ref):
        for index in range(length // own):
            rows = pl.ds(pl.multiple_of(places_ref[index] * own, own), own)
            if (index + 1) * own <= near_ref.shape[0]:
                yield rows, near_ref[index * own : (index + 1) * own, :]
            else:
                yield rows, far_ref[...]

    @pl.when(head == 0)
    def _():
        for index, down in enumerate((down_own, down_left, down_right, down_far)):
            rows = pl.ds(pl.multiple_of(places_ref[index] * own, own), own)
            downs[rows, :] = down[...]
        for rows, k in each_chunk(k_near_ref, k_far_ref):
            k = turned(k.astype(bf16).astype(f32), cos_ref[rows, :], sin_ref[rows, :])
            keys[rows, :] = k.astype(bf16)
        for rows, v in each_chunk(v_near_ref, v_far_ref):
            v = v + ADAPTER_SCALE * dot(downs[rows, rank:], up_v_ref[...])
            values[rows, :] = v.astype(bf16)
        keys_t[...] = keys[...].astype(f32).T.astype(bf16)
        values_t[...] = values[...].astype(f32).T.astype(bf16)
        grad_values_t[...] = jnp.zeros_like(grad_values_t)
        mid_q[...] = jnp.zeros_like(mid_q)

    up_q = up_q_ref[...]
    for rows, q in each_chunk(q_near_ref, q_far_ref):
        q = (q + ADAPTER_SCALE * dot(downs[rows, :rank], up_q)).astype(bf16)
        queries[rows, :] = turned(q.astype(f32), cos_ref[rows, :], sin_ref[rows, :]).astype(bf16)
    half = own // 2

    def spots():
        starts = [pl.multiple_of(places_ref[index] * own, own) for index in range(4)]
        low = pl.multiple_of(starts[3] + half, half)
        return [pl.ds(start, own) for start in starts[:3]] + [pl.ds(starts[3], half), pl.ds(low, half)]

    for rows, part in zip(spots(), (grad_own, grad_left, grad_right, grad_top, grad_low)):
        grads[rows, :] = part[...]
    spans = [(pl.ds(i * block, block), (i + 1) * block) for i in reversed(range(length // block))]
    row_ids = lax.broadcasted_iota(jnp.int32, (block, block), 0)
    col_ids = lax.broadcasted_iota(jnp.int32, (block, block), 1)
    causal = row_ids >= col_ids
    all_scores = [dot(queries[rows, :], keys_t[:, :seen]) for rows, seen in spans]
    softmaxes = []
    for (rows, seen), scores in zip(spans, all_scores):
        diagonal = jnp.where(causal, scores[:, seen - block :], -1e30)
        if seen > block:
            scores = jnp.concatenate([scores[:, : seen - block], diagonal], 1)
        else:
            scores = diagonal
        weights = jnp.exp2((scores - jnp.max(scores, axis=-1, keepdims=True)) * to_exp2)
        inverse = 1.0 / jnp.sum(weights, axis=-1, keepdims=True)
        softmaxes.append((weights, inverse, weights.astype(bf16)))
    grad_qs = []
    for (rows, seen), (weights, inverse, rounded), grad_p in zip(spans, softmaxes, [None] * 3):
        attended = dot(rounded, values[:seen, :]) * inverse
        outs[rows, :] = attended.astype(bf16)
        grad_f32 = grads[rows, :].astype(f32)
        along = jnp.sum(grad_f32 * attended, axis=-1, keepdims=True)
        grad_p = dot(grads[rows, :], values_t[:, :seen])
        grad_scores = (weights * (grad_p - along)).astype(bf16)
        grad_qs.append(dot(grad_scores, keys[:seen, :]) * (inverse * scale))
        grad_values_t[:, :seen] += dot((grad_f32 * inverse).T.astype(bf16), rounded)
    grad_b = jnp.zeros(grad_b_q_ref.shape, f32)
    for (rows, seen), grad_q in zip(spans, grad_qs):
        grad_q = turned(grad_q.astype(bf16).astype(f32), cos_ref[rows, :], -sin_ref[rows, :])
        grad_q = grad_q.astype(bf16)
        grad_b += dot_general(downs[rows, :rank], grad_q, TN)
        mid_q[:, rows] += dot_general(up_q, grad_q, NT)
    grad_b_q_ref[...] = ADAPTER_SCALE * grad_b
    for rows, part in zip(spots(), (out_own, out_left, out_right, out_top, out_low)):
        part[...] = outs[rows, :]

    @pl.when(head == last)
    def _():
        grad_v = grad_values_t[...].T.astype(bf16)
        grad_b_v_ref[...] = ADAPTER_SCALE * dot_general(downs[:, rank:], grad_v, TN)
        mid_ref[:rank, :] = mid_q[...]
        mid_ref[rank:, :] = dot_general(up_v_ref[...], grad_v, NT)


def attention(places, near, far, downs, up_q, up_v, grads, cosine, sine):
    close, own = near.shape[0], far.shape[0]
    length = close + own
    rank = up_q.shape[0]
    heads = up_q.shape[1] // HD
    whole = lambda h, p: (0, 0)
    column = lambda h, p: (0, h)
    f32, bf16 = jnp.float32, jnp.bfloat16
    pairs = []
    for index in (column, lambda h, p: (0, heads), lambda h, p: (0, heads + 1)):
        pairs += [pl.BlockSpec((close, HD), index), pl.BlockSpec((own, HD), index)]
    return pl.pallas_call(
        functools.partial(attention_kernel, 256),
        grid_spec=pltpu.PrefetchScalarGridSpec(
            num_scalar_prefetch=1,
            grid=(heads,),
            in_specs=pairs
            + [
                *[pl.BlockSpec((own, 2 * rank), whole)] * 4,
                pl.BlockSpec((rank, HD), column),
                pl.BlockSpec((rank, HD), whole),
                pl.BlockSpec((length, HD), whole),
                pl.BlockSpec((length, HD), whole),
            ]
            + [pl.BlockSpec((part.shape[0], HD), column) for part in grads],
            out_specs=[pl.BlockSpec((part.shape[0], HD), column) for part in grads]
            + [
                pl.BlockSpec((rank, HD), column),
                pl.BlockSpec((rank, HD), whole),
                pl.BlockSpec((2 * rank, length), whole),
            ],
            scratch_shapes=[
                pltpu.VMEM((length, HD), bf16),
                pltpu.VMEM((length, HD), bf16),
                pltpu.VMEM((length, HD), bf16),
                pltpu.VMEM((length, HD), bf16),
                pltpu.VMEM((HD, length), bf16),
                pltpu.VMEM((length, HD), bf16),
                pltpu.VMEM((HD, length), bf16),
                pltpu.VMEM((length, 2 * rank), bf16),
                pltpu.VMEM((HD, length), f32),
                pltpu.VMEM((rank, length), f32),
            ],
        ),
        out_shape=[jax.ShapeDtypeStruct(part.shape, bf16) for part in grads]
        + [
            jax.ShapeDtypeStruct((rank, heads * HD), f32),
            jax.ShapeDtypeStruct((rank, HD), f32),
            jax.ShapeDtypeStruct((2 * rank, length), f32),
        ],
        compiler_params=pltpu.CompilerParams(dimension_semantics=("arbitrary",)),
        name="attention",
    )(
        places, near, far, near, far, near, far,
        *downs, up_q, up_v, cosine, sine, *grads,
    )


def coordinates():
    dp, fsdp = lax.axis_index("dp"), lax.axis_index("fsdp")
    return dp // 2 * 2 + fsdp % 2, fsdp // 2, dp % 2


def position(x, z, c):
    return (x // 2 * 2 + c) * 8 + z * 2 + x % 2


def moves(dx=0, dz=0, dc=0):
    return [
        (position(x, z, c), position((x + dx) % 4, (z + dz) % 4, (c + dc) % 2))
        for x in range(4)
        for z in range(4)
        for c in range(2)
    ]


def send(array, dx=0, dz=0, dc=0):
    return lax.ppermute(array, WHERE, moves(dx, dz, dc))


def around(array, **step):
    back = {axis: -size for axis, size in step.items()}
    before, after = send(array, **step), send(array, **back)
    half = array.shape[0] // 2
    top, low = send(before[:half], **step), send(after[half:], **back)
    return before, after, top, low


def around_halves(first, second, **step):
    back = {axis: -size for axis, size in step.items()}
    before_first, after_second = send(first, **step), send(second, **back)
    before_second, after_first = send(second, **step), send(first, **back)
    far_first, far_second = send(before_first, **step), send(after_second, **back)
    return before_first, after_second, before_second, after_first, far_first, far_second


def join_kernel(at_ref, own, before, after, top, low, out_ref, first_ref, second_ref, sem):
    at = at_ref[0]
    cut = top.shape[0]
    far = out_ref.at[(at + 2) % 4]
    copies = [
        pltpu.make_async_copy(own, out_ref.at[at], sem.at[0]),
        pltpu.make_async_copy(before, out_ref.at[(at + 3) % 4], sem.at[1]),
        pltpu.make_async_copy(after, out_ref.at[(at + 1) % 4], sem.at[2]),
        pltpu.make_async_copy(top, far.at[pl.ds(0, cut)], sem.at[3]),
        pltpu.make_async_copy(low, far.at[pl.ds(cut, cut)], sem.at[4]),
    ]
    for copy in copies:
        copy.start()
    for copy in copies:
        copy.wait()
    first_ref[...] = out_ref[:2]
    second_ref[...] = out_ref[2:]


def joined(own, pieces, at):
    anywhere = pl.BlockSpec(memory_space=pl.ANY)
    return pl.pallas_call(
        join_kernel,
        grid_spec=pltpu.PrefetchScalarGridSpec(
            num_scalar_prefetch=1,
            grid=(1,),
            in_specs=[anywhere] * 5,
            out_specs=[pl.BlockSpec((n, *own.shape), lambda i, p: (0, 0, 0)) for n in (4, 2, 2)],
            scratch_shapes=[pltpu.SemaphoreType.DMA((5,))],
        ),
        out_shape=[jax.ShapeDtypeStruct((n, *own.shape), own.dtype) for n in (4, 2, 2)],
        name="join",
    )(at.reshape(1).astype(jnp.int32), own, *pieces)


def gather_weights(shard, x, z, c):
    rows, _ = shard.shape
    half = rows // 2

    along_x, *halves_x = joined(shard[:half], around(shard[:half], dx=1), x)
    along_z, *halves_z = joined(shard[half:], around(shard[half:], dz=1), z)
    from_z = around_halves(*halves_x, dz=1)
    from_x = around_halves(*halves_z, dx=1)
    pieces, starts = [], []

    def add(piece, blocks, core, second):
        pieces.append(piece)
        starts.extend(position(x, z, core) * rows + second * half for x, z in blocks)

    first, second = range(2), range(2, 4)
    spans = (range(4), first, second, second, first, first, second)
    turns = (0, -1, 1, -1, 1, 2, 2)
    for k in range(len(turns)):
        for other in (False, True):
            core = 1 - c if other else c
            piece = (along_x, *from_z)[k]
            at = (z + turns[k]) % 4
            piece = send(piece, dc=1) if other else piece
            add(piece, [(i, at) for i in spans[k]], core, 0)
            piece = (along_z, *from_x)[k]
            at = (x + turns[k]) % 4
            piece = send(piece, dc=1) if other else piece
            add(piece, [(at, i) for i in spans[k]], core, 1)
    return pieces, jnp.stack([jnp.asarray(start, jnp.int32) for start in starts])


def pick(array, index):
    return lax.dynamic_index_in_dim(array, index, 0, keepdims=False)


def placed(array, at, parts):
    size = len(parts) + 1
    line = jnp.zeros((size, *array.shape), array.dtype)
    for k, part in enumerate((array, *parts)):
        line = lax.dynamic_update_index_in_dim(line, part, (at + size - k) % size, 0)
    return line


def reduce(keep, give, x, z):
    total = keep + send(give, dc=1)
    others = [send(pick(total, (x + k) % 4), dx=k) for k in (1, 2, 3)]
    total = (pick(total, x) + others[0] + others[1] + others[2]).astype(jnp.bfloat16)
    parts = placed(total, z, [send(total, dz=k) for k in (1, 2, 3)])
    return parts.astype(jnp.float32).sum(axis=0).astype(jnp.bfloat16)


def all_gather(mine, me, x, c):
    first = mine[..., :SHARED]
    first = placed(first, me, [lax.ppermute(first, "tensor", ring(4, k)) for k in (1, 2, 3)])
    mine = jnp.concatenate([*first, mine[..., SHARED:]], -1)
    mine = placed(mine, x, [send(mine, dx=k) for k in (1, 2, 3)])
    return placed(mine, c, [send(mine, dc=1)])


SHARED, LANES = 256, 384


def feature_kernel(
    places_ref, mid0, mid1, mid2, mid3, *refs
):
    parts, (grad_q_ref, grad_v_ref, keep_ref, give_ref, mids, packed) = refs[:-6], refs[-6:]
    f32, bf16 = jnp.float32, jnp.bfloat16
    half = parts[0].shape[0]
    mids[...] = (mid0[...] + mid1[...] + mid2[...] + mid3[...]).T.astype(bf16)
    total = jnp.zeros((mids.shape[1], parts[0].shape[1]), f32)
    for index, part in enumerate(parts):
        start = places_ref[index // 2] * 2 * half + index % 2 * half
        mid = mids[pl.ds(pl.multiple_of(start, half), half), :]
        total = total + lax.dot_general(mid, part[...], TN, preferred_element_type=f32)
    total = total * ADAPTER_SCALE
    packed[:, :, SHARED:] = jnp.zeros((32, 8, LANES - SHARED), f32)
    for chunk in range(32):
        top, left = chunk // 8, chunk % 8
        packed[chunk, :, :SHARED] = total[top * 8 : top * 8 + 8, left * 256 : left * 256 + 256]
        packed[chunk, :4, SHARED:] = grad_q_ref[top * 4 : top * 4 + 4, left * 128 : left * 128 + 128]
        if chunk < 16:
            packed[chunk, 4:5, SHARED:] = grad_v_ref[chunk : chunk + 1, :]
    core = places_ref[4]
    keep_ref[...] = packed[pl.ds(core * 16, 16)]
    give_ref[...] = packed[pl.ds((1 - core) * 16, 16)]


def feature_gradient(places, mids, parts, grad_b_q, grad_b_v):
    half, width = parts[0].shape
    part = width // 4
    whole = lambda i, p: (0, 0)
    out = pl.BlockSpec((16, 8, LANES), lambda i, p: (0, 0, 0))
    keep, give = pl.pallas_call(
        feature_kernel,
        grid_spec=pltpu.PrefetchScalarGridSpec(
            num_scalar_prefetch=1,
            grid=(1,),
            in_specs=[
                *[pl.BlockSpec(mids[0].shape, whole)] * 4,
                *[pl.BlockSpec((half, part), lambda i, p: (0, p[0]))] * len(parts),
                pl.BlockSpec(grad_b_q.shape, whole),
                pl.BlockSpec(grad_b_v.shape, whole),
            ],
            out_specs=[out, out],
            scratch_shapes=[
                pltpu.VMEM(mids[0].shape[::-1], jnp.bfloat16),
                pltpu.VMEM((32, 8, LANES), jnp.float32),
            ],
        ),
        out_shape=[jax.ShapeDtypeStruct((16, 8, LANES), jnp.float32)] * 2,
        name="features",
    )(places, *mids, *parts, grad_b_q, grad_b_v)
    return keep.reshape(4, 4, 8, LANES), give.reshape(4, 4, 8, LANES)


def unpack_kernel(all_ref, a_query_ref, a_value_ref, grad_q_ref, grad_v_ref):
    f32 = jnp.float32
    for chunk in range(32):
        top, left = chunk // 8, chunk % 8
        target = (a_query_ref, a_value_ref)[top // 2]
        row = top % 2 * 8
        for y in range(4):
            lane = y * 2048 + left * 256
            piece = all_ref[chunk, :, y * SHARED : y * SHARED + SHARED].astype(f32)
            target[row : row + 8, lane : lane + 256] = piece
        mine = all_ref[chunk, :, 4 * SHARED :].astype(f32)
        grad_q_ref[top * 4 : top * 4 + 4, left * 128 : left * 128 + 128] = mine[:4]
        if chunk < 16:
            grad_v_ref[chunk : chunk + 1, :] = mine[4:5]


def unpack(everything, rank):
    everything = everything.reshape(32, 8, -1)
    shapes = ((rank, 8192), (rank, 8192), (rank, 1024), (rank, 128))
    return pl.pallas_call(
        unpack_kernel,
        out_shape=[jax.ShapeDtypeStruct(s, jnp.float32) for s in shapes],
        name="unpack",
    )(everything)


def local(tokens, norm_gain, w_qkv, a_query, query_up_adapter, a_value, value_up_adapter, out_grad):
    f32, bf16 = jnp.float32, jnp.bfloat16
    size = lax.axis_size("tensor")
    me = lax.axis_index("tensor")
    rank = a_query.shape[1]
    own = out_grad.shape[1]
    half = own // 2
    x, z, c = coordinates()
    ahead, behind = ring(size, 1), ring(size, -1)
    right, left, across = (me + 1) % size, (me + size - 1) % size, (me + 2) % size

    def along(array, pairs):
        return lax.ppermute(array, "tensor", pairs)

    width = out_grad.shape[2] // size
    group = lambda at: lax.dynamic_slice(out_grad[0], (0, at * width), (own, width))
    cross = group(across)
    grads = (
        group(me),
        along(group(right), ahead),
        along(group(left), behind),
        along(along(cross[:half], ahead), ahead),
        along(along(cross[half:], behind), behind),
    )
    pieces, starts = gather_weights(w_qkv, x, z, c)

    top = normalize(tokens[0], norm_gain, 0, half, 32)
    low = normalize(tokens[0], norm_gain, half, half, 32)
    left_top = along(top, ahead)
    right_low = along(low, behind)
    left_low = along(low, ahead)
    right_top = along(top, behind)
    far_top = along(left_top, ahead)
    far_low = along(right_low, behind)
    near, far = (top, low, left_top, left_low, right_top, right_low), (far_top, far_low)

    adapters = jnp.concatenate([a_query, a_value], 1)
    down = jnp.concatenate(
        [jnp.dot(part, adapters, preferred_element_type=f32).astype(bf16) for part in (top, low)]
    )
    places = jnp.stack([me, left, right, across, c]).astype(jnp.int32)
    cosine, sine = rotary_tables(own * size)
    down, places, starts, cosine, sine = lax.optimization_barrier(
        (down, places, starts, cosine, sine)
    )
    downs = [down] + [along(down, ring(size, step)) for step in (1, -1, 2)]
    near_projected = project(near, starts, pieces, 4)
    far_projected = project(far, starts, pieces, 8)
    mine, for_left, for_right, for_top, for_low, grad_b_q, grad_b_v, mid = attention(
        places, near_projected, far_projected, downs,
        query_up_adapter, value_up_adapter, grads, cosine, sine,
    )

    mids = [mid] + [along(mid, ring(size, k)) for k in (1, 2, 3)]
    out = jnp.zeros((own, out_grad.shape[2]), bf16)
    for piece, row, source in (
        (mine, 0, me),
        (along(for_right, ahead), 0, left),
        (along(for_left, behind), 0, right),
        (along(along(for_top, ahead), ahead), 0, across),
        (along(along(for_low, behind), behind), half, across),
    ):
        out = lax.dynamic_update_slice(out, piece, (row, source * width))
    keep, give = feature_gradient(places, mids, near + far, grad_b_q, grad_b_v)
    summed = reduce(keep, give, x, z)
    grad_a_q, grad_a_v, grad_b_q, grad_b_v = unpack(all_gather(summed, me, x, c), rank)
    return out[None], grad_a_q.T, grad_b_q, grad_a_v.T, grad_b_v


def solution(mesh):
    return jax.shard_map(
        local,
        mesh=mesh,
        in_specs=(
            P(("dp", "fsdp"), "tensor", None),
            P(),
            P(("dp", "fsdp"), "tensor"),
            P(),
            P(None, "tensor"),
            P(),
            P(None, "tensor"),
            P(("dp", "fsdp"), "tensor", None),
        ),
        out_specs=(
            P(("dp", "fsdp"), "tensor", None),
            P(),
            P(None, "tensor"),
            P(),
            P(None, "tensor"),
        ),
        check_vma=False,
    )
```

```python
import functools
import math

import jax
import jax.numpy as jnp
from jax import lax
from jax.experimental import pallas as pl
from jax.experimental.pallas import tpu as pltpu
from jax.sharding import PartitionSpec as P


HD = 128


EPSILON = 1e-05
ADAPTER_SCALE = 2.0
ROPE_BASE = 500000.0
WHERE = ("dp", "fsdp")
NT = (((1,), (1,)), ((), ()))
TN = (((0,), (0,)), ((), ()))


def ring(size, step):
    return [(i, (i + step) % size) for i in range(size)]


def normalize_kernel(rows_ref, gain_ref, out_ref):
    widened = rows_ref[...].astype(jnp.float32)
    mean_square = jnp.mean(widened * widened, axis=-1, keepdims=True)
    normed = widened * lax.rsqrt(mean_square + EPSILON) * gain_ref[...]
    out_ref[...] = normed.astype(jnp.bfloat16)


def normalize(rows, norm_gain, first, count, block):
    width = rows.shape[1]
    return pl.pallas_call(
        normalize_kernel,
        grid=(count // block,),
        in_specs=[
            pl.BlockSpec((block, width), lambda i: (first // block + i, 0)),
            pl.BlockSpec((1, width), lambda i: (0, 0)),
        ],
        out_specs=pl.BlockSpec((block, width), lambda i: (i, 0)),
        out_shape=jax.ShapeDtypeStruct((count, width), jnp.bfloat16),
        compiler_params=pltpu.CompilerParams(dimension_semantics=("arbitrary",)),
        name="normalize",
    )(rows, norm_gain.reshape(1, width))


AHEAD = 3


def project_kernel(turns, n_rows, starts_ref, *refs):
    n_pieces = sum(len(turn) for turn in turns)
    rows_refs, pieces = refs[:n_rows], refs[n_rows : n_rows + n_pieces]
    out_ref, rows, weights, rows_sem, weights_sem = refs[n_rows + n_pieces :]
    deep = weights.shape[0] // len(turns)
    depth = weights.shape[0] // starts_ref.shape[0]
    blocks = deep // depth

    def fetch(turn):
        place = turn * deep
        for piece, count in turns[turn]:
            pltpu.make_async_copy(
                pieces[piece], weights.at[pl.ds(place, count)], weights_sem.at[turn]
            ).start()
            place += count

    row_copies = []
    for index, ref in enumerate(rows_refs):
        count = ref.shape[0]
        row_copies.append(
            pltpu.make_async_copy(
                ref, rows.at[pl.ds(index * count, count)], rows_sem.at[index]
            )
        )
        row_copies[-1].start()
    for turn in range(AHEAD):
        fetch(turn)
    out_ref[...] = jnp.zeros_like(out_ref)
    for copy in row_copies:
        copy.wait()

    def step(turn, carry):
        for later in range(AHEAD, len(turns)):

            @pl.when(turn + AHEAD == later)
            def _(later=later):
                fetch(later)

        here = weights.at[pl.ds(pl.multiple_of(turn * deep, deep), deep)]
        pltpu.make_async_copy(here, here, weights_sem.at[turn]).wait()
        columns = [
            rows[:, pl.ds(pl.multiple_of(starts_ref[turn * blocks + k], depth), depth)]
            for k in range(blocks)
        ]
        out_ref[...] += jnp.dot(
            jnp.concatenate(columns, 1), here[...], preferred_element_type=jnp.float32
        )
        return carry

    lax.fori_loop(0, len(turns), step, 0)


def project(rows, starts, pieces, blocks):
    depth, cols = pieces[0].shape[1:]
    sizes = [piece.shape[0] for piece in pieces]
    count, width = sum(part.shape[0] for part in rows), rows[0].shape[1]
    anywhere = pl.BlockSpec(memory_space=pl.ANY)
    turns, filled = [[]], 0
    for index, size in enumerate(sizes):
        if filled == blocks:
            turns.append([])
            filled = 0
        turns[-1].append((index, size * depth))
        filled += size
    return pl.pallas_call(
        functools.partial(project_kernel, turns, len(rows)),
        grid_spec=pltpu.PrefetchScalarGridSpec(
            num_scalar_prefetch=1,
            grid=(1,),
            in_specs=[anywhere] * (len(rows) + len(pieces)),
            out_specs=pl.BlockSpec((count, cols), lambda i, p: (0, 0)),
            scratch_shapes=[
                pltpu.VMEM((count, width), jnp.bfloat16),
                pltpu.VMEM((sum(sizes) * depth, cols), jnp.bfloat16),
                pltpu.SemaphoreType.DMA((len(rows),)),
                pltpu.SemaphoreType.DMA((len(turns),)),
            ],
        ),
        out_shape=jax.ShapeDtypeStruct((count, cols), jnp.float32),
        name="project",
    )(starts, *rows, *[piece.reshape(-1, cols) for piece in pieces])


def rotary_tables(sequence_length):
    half_dim = HD // 2
    positions = jnp.arange(sequence_length, dtype=jnp.float32)[:, None]
    inv_freq = ROPE_BASE ** (-jnp.arange(half_dim, dtype=jnp.float32) / half_dim)
    angles = positions * inv_freq
    cosine = jnp.cos(angles)
    sine = jnp.sin(angles)
    return jnp.concatenate([cosine, cosine], 1), jnp.concatenate([-sine, sine], 1)


def attention_kernel(
    block, places_ref,
    q_near_ref, q_far_ref, k_near_ref, k_far_ref, v_near_ref, v_far_ref,
    down_own, down_left, down_right, down_far, up_q_ref, up_v_ref, cos_ref, sin_ref,
    grad_own, grad_left, grad_right, grad_top, grad_low,
    out_own, out_left, out_right, out_top, out_low, grad_b_q_ref, grad_b_v_ref, mid_ref,
    queries, grads, outs, keys, keys_t, values, values_t, downs, grad_values_t, mid_q,
):
    head = pl.program_id(0)
    last = pl.num_programs(0) - 1
    length = outs.shape[0]
    own = q_far_ref.shape[0]
    rank = up_q_ref.shape[0]
    f32, bf16 = jnp.float32, jnp.bfloat16
    dot = functools.partial(jnp.dot, preferred_element_type=f32)
    dot_general = functools.partial(lax.dot_general, preferred_element_type=f32)
    scale = 1.0 / math.sqrt(HD)
    to_exp2 = scale * math.log2(math.e)

    def turned(x, cosine, sine):
        return x * cosine + pltpu.roll(x, HD // 2, 1) * sine

    def each_chunk(near_ref, far_ref):
        for index in range(length // own):
            rows = pl.ds(pl.multiple_of(places_ref[index] * own, own), own)
            if (index + 1) * own <= near_ref.shape[0]:
                yield rows, near_ref[index * own : (index + 1) * own, :]
            else:
                yield rows, far_ref[...]

    @pl.when(head == 0)
    def _():
        for index, down in enumerate((down_own, down_left, down_right, down_far)):
            rows = pl.ds(pl.multiple_of(places_ref[index] * own, own), own)
            downs[rows, :] = down[...]
        for rows, k in each_chunk(k_near_ref, k_far_ref):
            k = turned(k.astype(bf16).astype(f32), cos_ref[rows, :], sin_ref[rows, :])
            keys[rows, :] = k.astype(bf16)
        for rows, v in each_chunk(v_near_ref, v_far_ref):
            v = v + ADAPTER_SCALE * dot(downs[rows, rank:], up_v_ref[...])
            values[rows, :] = v.astype(bf16)
        keys_t[...] = keys[...].astype(f32).T.astype(bf16)
        values_t[...] = values[...].astype(f32).T.astype(bf16)
        grad_values_t[...] = jnp.zeros_like(grad_values_t)
        mid_q[...] = jnp.zeros_like(mid_q)

    up_q = up_q_ref[...]
    for rows, q in each_chunk(q_near_ref, q_far_ref):
        q = (q + ADAPTER_SCALE * dot(downs[rows, :rank], up_q)).astype(bf16)
        queries[rows, :] = turned(q.astype(f32), cos_ref[rows, :], sin_ref[rows, :]).astype(bf16)
    half = own // 2

    def spots():
        starts = [pl.multiple_of(places_ref[index] * own, own) for index in range(4)]
        low = pl.multiple_of(starts[3] + half, half)
        return [pl.ds(start, own) for start in starts[:3]] + [pl.ds(starts[3], half), pl.ds(low, half)]

    for rows, part in zip(spots(), (grad_own, grad_left, grad_right, grad_top, grad_low)):
        grads[rows, :] = part[...]
    spans = [(pl.ds(i * block, block), (i + 1) * block) for i in reversed(range(length // block))]
    row_ids = lax.broadcasted_iota(jnp.int32, (block, block), 0)
    col_ids = lax.broadcasted_iota(jnp.int32, (block, block), 1)
    causal = row_ids >= col_ids
    all_scores = [dot(queries[rows, :], keys_t[:, :seen]) for rows, seen in spans]
    softmaxes = []
    for (rows, seen), scores in zip(spans, all_scores):
        diagonal = jnp.where(causal, scores[:, seen - block :], -1e30)
        if seen > block:
            scores = jnp.concatenate([scores[:, : seen - block], diagonal], 1)
        else:
            scores = diagonal
        weights = jnp.exp2((scores - jnp.max(scores, axis=-1, keepdims=True)) * to_exp2)
        inverse = 1.0 / jnp.sum(weights, axis=-1, keepdims=True)
        softmaxes.append((weights, inverse, weights.astype(bf16)))
    grad_qs = []
    for (rows, seen), (weights, inverse, rounded), grad_p in zip(spans, softmaxes, [None] * 3):
        attended = dot(rounded, values[:seen, :]) * inverse
        outs[rows, :] = attended.astype(bf16)
        grad_f32 = grads[rows, :].astype(f32)
        along = jnp.sum(grad_f32 * attended, axis=-1, keepdims=True)
        grad_p = dot(grads[rows, :], values_t[:, :seen])
        grad_scores = (weights * (grad_p - along)).astype(bf16)
        grad_qs.append(dot(grad_scores, keys[:seen, :]) * (inverse * scale))
        grad_values_t[:, :seen] += dot((grad_f32 * inverse).T.astype(bf16), rounded)
    grad_b = jnp.zeros(grad_b_q_ref.shape, f32)
    for (rows, seen), grad_q in zip(spans, grad_qs):
        grad_q = turned(grad_q.astype(bf16).astype(f32), cos_ref[rows, :], -sin_ref[rows, :])
        grad_q = grad_q.astype(bf16)
        grad_b += dot_general(downs[rows, :rank], grad_q, TN)
        mid_q[:, rows] += dot_general(up_q, grad_q, NT)
    grad_b_q_ref[...] = ADAPTER_SCALE * grad_b
    for rows, part in zip(spots(), (out_own, out_left, out_right, out_top, out_low)):
        part[...] = outs[rows, :]

    @pl.when(head == last)
    def _():
        grad_v = grad_values_t[...].T.astype(bf16)
        grad_b_v_ref[...] = ADAPTER_SCALE * dot_general(downs[:, rank:], grad_v, TN)
        mid_ref[:rank, :] = mid_q[...]
        mid_ref[rank:, :] = dot_general(up_v_ref[...], grad_v, NT)


def attention(places, near, far, downs, up_q, up_v, grads, cosine, sine):
    close, own = near.shape[0], far.shape[0]
    length = close + own
    rank = up_q.shape[0]
    heads = up_q.shape[1] // HD
    whole = lambda h, p: (0, 0)
    column = lambda h, p: (0, h)
    f32, bf16 = jnp.float32, jnp.bfloat16
    pairs = []
    for index in (column, lambda h, p: (0, heads), lambda h, p: (0, heads + 1)):
        pairs += [pl.BlockSpec((close, HD), index), pl.BlockSpec((own, HD), index)]
    return pl.pallas_call(
        functools.partial(attention_kernel, 256),
        grid_spec=pltpu.PrefetchScalarGridSpec(
            num_scalar_prefetch=1,
            grid=(heads,),
            in_specs=pairs
            + [
                *[pl.BlockSpec((own, 2 * rank), whole)] * 4,
                pl.BlockSpec((rank, HD), column),
                pl.BlockSpec((rank, HD), whole),
                pl.BlockSpec((length, HD), whole),
                pl.BlockSpec((length, HD), whole),
            ]
            + [pl.BlockSpec((part.shape[0], HD), column) for part in grads],
            out_specs=[pl.BlockSpec((part.shape[0], HD), column) for part in grads]
            + [
                pl.BlockSpec((rank, HD), column),
                pl.BlockSpec((rank, HD), whole),
                pl.BlockSpec((2 * rank, length), whole),
            ],
            scratch_shapes=[
                pltpu.VMEM((length, HD), bf16),
                pltpu.VMEM((length, HD), bf16),
                pltpu.VMEM((length, HD), bf16),
                pltpu.VMEM((length, HD), bf16),
                pltpu.VMEM((HD, length), bf16),
                pltpu.VMEM((length, HD), bf16),
                pltpu.VMEM((HD, length), bf16),
                pltpu.VMEM((length, 2 * rank), bf16),
                pltpu.VMEM((HD, length), f32),
                pltpu.VMEM((rank, length), f32),
            ],
        ),
        out_shape=[jax.ShapeDtypeStruct(part.shape, bf16) for part in grads]
        + [
            jax.ShapeDtypeStruct((rank, heads * HD), f32),
            jax.ShapeDtypeStruct((rank, HD), f32),
            jax.ShapeDtypeStruct((2 * rank, length), f32),
        ],
        compiler_params=pltpu.CompilerParams(dimension_semantics=("arbitrary",)),
        name="attention",
    )(
        places, near, far, near, far, near, far,
        *downs, up_q, up_v, cosine, sine, *grads,
    )


def coordinates():
    dp, fsdp = lax.axis_index("dp"), lax.axis_index("fsdp")
    return dp // 2 * 2 + fsdp % 2, fsdp // 2, dp % 2


def position(x, z, c):
    return (x // 2 * 2 + c) * 8 + z * 2 + x % 2


def moves(dx=0, dz=0, dc=0):
    return [
        (position(x, z, c), position((x + dx) % 4, (z + dz) % 4, (c + dc) % 2))
        for x in range(4)
        for z in range(4)
        for c in range(2)
    ]


def send(array, dx=0, dz=0, dc=0):
    return lax.ppermute(array, WHERE, moves(dx, dz, dc))


def around(array, **step):
    back = {axis: -size for axis, size in step.items()}
    before, after = send(array, **step), send(array, **back)
    half = array.shape[0] // 2
    top, low = send(before[:half], **step), send(after[half:], **back)
    return before, after, top, low


def around_halves(first, second, **step):
    back = {axis: -size for axis, size in step.items()}
    before_first, after_second = send(first, **step), send(second, **back)
    before_second, after_first = send(second, **step), send(first, **back)
    far_first, far_second = send(before_first, **step), send(after_second, **back)
    return before_first, after_second, before_second, after_first, far_first, far_second


def join_kernel(at_ref, own, before, after, top, low, out_ref, first_ref, second_ref, sem):
    at = at_ref[0]
    cut = top.shape[0]
    far = out_ref.at[(at + 2) % 4]
    copies = [
        pltpu.make_async_copy(own, out_ref.at[at], sem.at[0]),
        pltpu.make_async_copy(before, out_ref.at[(at + 3) % 4], sem.at[1]),
        pltpu.make_async_copy(after, out_ref.at[(at + 1) % 4], sem.at[2]),
        pltpu.make_async_copy(top, far.at[pl.ds(0, cut)], sem.at[3]),
        pltpu.make_async_copy(low, far.at[pl.ds(cut, cut)], sem.at[4]),
    ]
    for copy in copies:
        copy.start()
    for copy in copies:
        copy.wait()
    first_ref[...] = out_ref[:2]
    second_ref[...] = out_ref[2:]


def joined(own, pieces, at):
    anywhere = pl.BlockSpec(memory_space=pl.ANY)
    return pl.pallas_call(
        join_kernel,
        grid_spec=pltpu.PrefetchScalarGridSpec(
            num_scalar_prefetch=1,
            grid=(1,),
            in_specs=[anywhere] * 5,
            out_specs=[pl.BlockSpec((n, *own.shape), lambda i, p: (0, 0, 0)) for n in (4, 2, 2)],
            scratch_shapes=[pltpu.SemaphoreType.DMA((5,))],
        ),
        out_shape=[jax.ShapeDtypeStruct((n, *own.shape), own.dtype) for n in (4, 2, 2)],
        name="join",
    )(at.reshape(1).astype(jnp.int32), own, *pieces)


def gather_weights(shard, x, z, c):
    rows, _ = shard.shape
    half = rows // 2

    along_x, *halves_x = joined(shard[:half], around(shard[:half], dx=1), x)
    along_z, *halves_z = joined(shard[half:], around(shard[half:], dz=1), z)
    from_z = around_halves(*halves_x, dz=1)
    from_x = around_halves(*halves_z, dx=1)
    pieces, starts = [], []

    def add(piece, blocks, core, second):
        pieces.append(piece)
        starts.extend(position(x, z, core) * rows + second * half for x, z in blocks)

    first, second = range(2), range(2, 4)
    spans = (range(4), first, second, second, first, first, second)
    turns = (0, -1, 1, -1, 1, 2, 2)
    for k in range(len(turns)):
        for other in (False, True):
            core = 1 - c if other else c
            piece = (along_x, *from_z)[k]
            at = (z + turns[k]) % 4
            piece = send(piece, dc=1) if other else piece
            add(piece, [(i, at) for i in spans[k]], core, 0)
            piece = (along_z, *from_x)[k]
            at = (x + turns[k]) % 4
            piece = send(piece, dc=1) if other else piece
            add(piece, [(at, i) for i in spans[k]], core, 1)
    return pieces, jnp.stack([jnp.asarray(start, jnp.int32) for start in starts])


def pick(array, index):
    return lax.dynamic_index_in_dim(array, index, 0, keepdims=False)


def placed(array, at, parts):
    size = len(parts) + 1
    line = jnp.zeros((size, *array.shape), array.dtype)
    for k, part in enumerate((array, *parts)):
        line = lax.dynamic_update_index_in_dim(line, part, (at + size - k) % size, 0)
    return line


def reduce(keep, give, x, z):
    total = keep + send(give, dc=1)
    parts = total.astype(jnp.bfloat16)
    others = [send(pick(parts, (x + k) % 4), dx=k) for k in (1, 2, 3)]
    for other in others:
        others_sum = other.astype(jnp.float32) + (0.0 if other is others[0] else others_sum)
    total = (pick(total, x) + others_sum).astype(jnp.bfloat16)
    parts = placed(total, z, [send(total, dz=k) for k in (1, 2, 3)])
    return parts.astype(jnp.float32).sum(axis=0).astype(jnp.bfloat16)


def all_gather(mine, me, x, c):
    first = mine[..., :SHARED]
    first = placed(first, me, [lax.ppermute(first, "tensor", ring(4, k)) for k in (1, 2, 3)])
    mine = jnp.concatenate([*first, mine[..., SHARED:]], -1)
    mine = placed(mine, x, [send(mine, dx=k) for k in (1, 2, 3)])
    return placed(mine, c, [send(mine, dc=1)])


SHARED, LANES = 256, 384


def feature_kernel(
    places_ref, mid0, mid1, mid2, mid3, *refs
):
    parts, (grad_q_ref, grad_v_ref, keep_ref, give_ref, mids, packed) = refs[:-6], refs[-6:]
    f32, bf16 = jnp.float32, jnp.bfloat16
    half = parts[0].shape[0]
    mids[...] = (mid0[...] + mid1[...] + mid2[...] + mid3[...]).T.astype(bf16)
    total = jnp.zeros((mids.shape[1], parts[0].shape[1]), f32)
    for index, part in enumerate(parts):
        start = places_ref[index // 2] * 2 * half + index % 2 * half
        mid = mids[pl.ds(pl.multiple_of(start, half), half), :]
        total = total + lax.dot_general(mid, part[...], TN, preferred_element_type=f32)
    total = total * ADAPTER_SCALE
    packed[:, :, SHARED:] = jnp.zeros((32, 8, LANES - SHARED), f32)
    for chunk in range(32):
        top, left = chunk // 8, chunk % 8
        packed[chunk, :, :SHARED] = total[top * 8 : top * 8 + 8, left * 256 : left * 256 + 256]
        packed[chunk, :4, SHARED:] = grad_q_ref[top * 4 : top * 4 + 4, left * 128 : left * 128 + 128]
        if chunk < 16:
            packed[chunk, 4:5, SHARED:] = grad_v_ref[chunk : chunk + 1, :]
    core = places_ref[4]
    keep_ref[...] = packed[pl.ds(core * 16, 16)]
    give_ref[...] = packed[pl.ds((1 - core) * 16, 16)]


def feature_gradient(places, mids, parts, grad_b_q, grad_b_v):
    half, width = parts[0].shape
    part = width // 4
    whole = lambda i, p: (0, 0)
    out = pl.BlockSpec((16, 8, LANES), lambda i, p: (0, 0, 0))
    keep, give = pl.pallas_call(
        feature_kernel,
        grid_spec=pltpu.PrefetchScalarGridSpec(
            num_scalar_prefetch=1,
            grid=(1,),
            in_specs=[
                *[pl.BlockSpec(mids[0].shape, whole)] * 4,
                *[pl.BlockSpec((half, part), lambda i, p: (0, p[0]))] * len(parts),
                pl.BlockSpec(grad_b_q.shape, whole),
                pl.BlockSpec(grad_b_v.shape, whole),
            ],
            out_specs=[out, out],
            scratch_shapes=[
                pltpu.VMEM(mids[0].shape[::-1], jnp.bfloat16),
                pltpu.VMEM((32, 8, LANES), jnp.float32),
            ],
        ),
        out_shape=[jax.ShapeDtypeStruct((16, 8, LANES), jnp.float32)] * 2,
        name="features",
    )(places, *mids, *parts, grad_b_q, grad_b_v)
    return keep.reshape(4, 4, 8, LANES), give.reshape(4, 4, 8, LANES)


def unpack_kernel(all_ref, a_query_ref, a_value_ref, grad_q_ref, grad_v_ref):
    f32 = jnp.float32
    for chunk in range(32):
        top, left = chunk // 8, chunk % 8
        target = (a_query_ref, a_value_ref)[top // 2]
        row = top % 2 * 8
        for y in range(4):
            lane = y * 2048 + left * 256
            piece = all_ref[chunk, :, y * SHARED : y * SHARED + SHARED].astype(f32)
            target[row : row + 8, lane : lane + 256] = piece
        mine = all_ref[chunk, :, 4 * SHARED :].astype(f32)
        grad_q_ref[top * 4 : top * 4 + 4, left * 128 : left * 128 + 128] = mine[:4]
        if chunk < 16:
            grad_v_ref[chunk : chunk + 1, :] = mine[4:5]


def unpack(everything, rank):
    everything = everything.reshape(32, 8, -1)
    shapes = ((rank, 8192), (rank, 8192), (rank, 1024), (rank, 128))
    return pl.pallas_call(
        unpack_kernel,
        out_shape=[jax.ShapeDtypeStruct(s, jnp.float32) for s in shapes],
        name="unpack",
    )(everything)


def local(tokens, norm_gain, w_qkv, a_query, query_up_adapter, a_value, value_up_adapter, out_grad):
    f32, bf16 = jnp.float32, jnp.bfloat16
    size = lax.axis_size("tensor")
    me = lax.axis_index("tensor")
    rank = a_query.shape[1]
    own = out_grad.shape[1]
    half = own // 2
    x, z, c = coordinates()
    ahead, behind = ring(size, 1), ring(size, -1)
    right, left, across = (me + 1) % size, (me + size - 1) % size, (me + 2) % size

    def along(array, pairs):
        return lax.ppermute(array, "tensor", pairs)

    width = out_grad.shape[2] // size
    group = lambda at: lax.dynamic_slice(out_grad[0], (0, at * width), (own, width))
    cross = group(across)
    grads = (
        group(me),
        along(group(right), ahead),
        along(group(left), behind),
        along(along(cross[:half], ahead), ahead),
        along(along(cross[half:], behind), behind),
    )
    pieces, starts = gather_weights(w_qkv, x, z, c)

    top = normalize(tokens[0], norm_gain, 0, half, 32)
    low = normalize(tokens[0], norm_gain, half, half, 32)
    left_top = along(top, ahead)
    right_low = along(low, behind)
    left_low = along(low, ahead)
    right_top = along(top, behind)
    far_top = along(left_top, ahead)
    far_low = along(right_low, behind)
    near, far = (top, low, left_top, left_low, right_top, right_low), (far_top, far_low)

    adapters = jnp.concatenate([a_query, a_value], 1)
    down = jnp.concatenate(
        [jnp.dot(part, adapters, preferred_element_type=f32).astype(bf16) for part in (top, low)]
    )
    places = jnp.stack([me, left, right, across, c]).astype(jnp.int32)
    cosine, sine = rotary_tables(own * size)
    down, places, starts, cosine, sine = lax.optimization_barrier(
        (down, places, starts, cosine, sine)
    )
    downs = [down] + [along(down, ring(size, step)) for step in (1, -1, 2)]
    near_projected = project(near, starts, pieces, 4)
    far_projected = project(far, starts, pieces, 8)
    mine, for_left, for_right, for_top, for_low, grad_b_q, grad_b_v, mid = attention(
        places, near_projected, far_projected, downs,
        query_up_adapter, value_up_adapter, grads, cosine, sine,
    )

    mids = [mid] + [along(mid, ring(size, k)) for k in (1, 2, 3)]
    out = jnp.zeros((own, out_grad.shape[2]), bf16)
    for piece, row, source in (
        (mine, 0, me),
        (along(for_right, ahead), 0, left),
        (along(for_left, behind), 0, right),
        (along(along(for_top, ahead), ahead), 0, across),
        (along(along(for_low, behind), behind), half, across),
    ):
        out = lax.dynamic_update_slice(out, piece, (row, source * width))
    keep, give = feature_gradient(places, mids, near + far, grad_b_q, grad_b_v)
    summed = reduce(keep, give, x, z)
    grad_a_q, grad_a_v, grad_b_q, grad_b_v = unpack(all_gather(summed, me, x, c), rank)
    return out[None], grad_a_q.T, grad_b_q, grad_a_v.T, grad_b_v


def solution(mesh):
    return jax.shard_map(
        local,
        mesh=mesh,
        in_specs=(
            P(("dp", "fsdp"), "tensor", None),
            P(),
            P(("dp", "fsdp"), "tensor"),
            P(),
            P(None, "tensor"),
            P(),
            P(None, "tensor"),
            P(("dp", "fsdp"), "tensor", None),
        ),
        out_specs=(
            P(("dp", "fsdp"), "tensor", None),
            P(),
            P(None, "tensor"),
            P(),
            P(None, "tensor"),
        ),
        check_vma=False,
    )
```
